32 devices in a mesh: section: 4 (over y, core), tensor: 8 (over z, x).
Axes of the slice: x: 2, y: 2, z: 4, core: 2. Of those that a mesh axis runs over, the one named last changes fastest.
Arguments:
- saved_inputs: bfloat16 [4, 4, 256, 1024], P('section', None, 'tensor'), may hold values from -6 to 6
- slot_index: int32 [4, 3], P('section'), may hold values from 0 to 3
- example_lengths: int32 [4, 3, 2], P('section'), may hold values from 1 to 192, 256 in all within a row
- first_grads: bfloat16 [4, 256, 1024], P('section', 'tensor'), may hold values from -6 to 6
- loss_grads: bfloat16 [2, 256, 1024], P(None, 'tensor'), may hold values from -6 to 6
- w_in: bfloat16 [4, 1024, 32768], P('section', None, 'tensor'), may hold values from -0.1875 to 0.1875
- w_out: bfloat16 [4, 32768, 1024], P('section', 'tensor'), may hold values from -0.03125 to 0.03125
Outputs:
- grad_in: bfloat16 [4, 1024, 32768], P('section', None, 'tensor')
- grad_out: bfloat16 [4, 32768, 1024], P('section', 'tensor')
- input_grads: bfloat16 [4, 3, 256, 1024], P('section', None, 'tensor')
The draws below stay inside these ranges and needn't reach their ends.
Inputs may be any that keep to these rules, and one draw needn't show every extreme that they name: `example_lengths`: the 2 lengths of one microbatch sum to 256.
All inputs are finite; a program needn't handle non-finite values.
Results may differ from the reference program's by a relative error of at most 0.0095.
Values may be sent and summed in bfloat16 or wider, within the bound.
A program may use at most 128 MiB of HBM per device.

```python
import math
import jax
import jax.numpy as jnp
import numpy as np
from jax import lax

D = 1024
FF = 32768
TOK_MB = 256
EXAMPLES = 2
SLOTS = 3
BUF = 4
MOST = 192
SECTIONS = 4


def plant(drawn, stream_key, low, high):
    shape = drawn.shape
    place = [jax.random.randint(jax.random.fold_in(stream_key, axis), (), 0, shape[axis]) for axis in range(len(shape))]
    drawn = drawn.at[tuple(place)].set(low)
    longest = shape.index(max(shape))
    place[longest] = (place[longest] + 1) % shape[longest]
    return drawn.at[tuple(place)].set(high)


def steps_of(own_key, dims, shards, smallest, high):
    def one(axis_at, shards_of):
        draws = jax.random.uniform(jax.random.fold_in(jax.random.fold_in(own_key, 6), axis_at), (shards_of,), jnp.float32, smallest / len(shards), high / len(shards))
        return jnp.repeat(jnp.exp(draws), dims[axis_at] // shards_of).reshape((-1,) + (1,) * (len(dims) - axis_at - 1))

    loudness = one(*shards[0])
    for cut in shards[1:]:
        loudness = loudness * one(*cut)
    return loudness


def split_up(count, total, most, lean):
    loads = [(1 << 20) // math.isqrt(grade ** lean) + 1 for grade in range(2, count + 1)]
    surplus, holding = total - most - (count - 1), [1] * (count - 1)
    while surplus > 0:
        free = [i for i in range(count - 1) if holding[i] < most]
        pool, left = sum([loads[i] for i in free]), surplus
        for i in free:
            addition = min(most - holding[i], max(1, left * loads[i] // pool), surplus)
            holding[i] = holding[i] + addition
            surplus = surplus - addition
    return np.array([most] + holding)


def uneven(rng, count, total, most, skew):
    if count == 2:
        one = jax.random.randint(rng, (), max(1, total - most), min(most, total - 1) + 1)
        return jnp.stack([one, total - one])
    sizes = jnp.asarray(split_up(count, total, most, skew), jnp.int32)
    pairs = (count - 1) // 2
    giver, sink = sizes[1:1 + 2 * pairs:2], sizes[2:2 + 2 * pairs:2]
    slack = jnp.minimum(giver - 1, most - sink)
    passed = jax.random.randint(jax.random.fold_in(rng, 1), (pairs,), 0, 1 << 20) % (slack + 1)
    sizes = sizes.at[1:1 + 2 * pairs:2].set(giver - passed).at[2:2 + 2 * pairs:2].set(sink + passed)
    return sizes[jax.random.permutation(jax.random.fold_in(rng, 2), count)]


def noise(rng, shape, spread, limit, split=(), kind=jnp.bfloat16):
    entries = spread * jax.random.normal(rng, shape, jnp.float32)
    if split:
        entries = entries * steps_of(rng, shape, split, -0.22, 0.18)
    return jnp.clip(entries, -limit, limit).astype(kind)


def setup_inputs(seed: int = 0) -> dict:
    key_of = jax.random.split(jax.random.key(seed), 8)
    saved_inputs = noise(key_of[0], (SECTIONS, BUF, TOK_MB, D), 1.0, 6.0, ((0, 4), (2, 8)))
    slot_index = plant(jax.random.randint(key_of[1], (SECTIONS, SLOTS), 0, BUF), jax.random.fold_in(key_of[1], 1), 0, BUF - 1).astype(jnp.int32)
    example_lengths = jax.vmap(lambda own: uneven(own, EXAMPLES, TOK_MB, MOST, 2))(jax.random.split(key_of[2], SECTIONS * SLOTS)).reshape((SECTIONS, SLOTS, EXAMPLES)).astype(jnp.int32)
    first_grads = noise(key_of[3], (SECTIONS, TOK_MB, D), 1.0, 6.0, ((0, 4), (1, 8)))
    loss_grads = noise(key_of[4], (SLOTS - 1, TOK_MB, D), 1.0, 6.0, ((1, 8),))
    w_in = noise(key_of[5], (SECTIONS, D, FF), D ** -0.5, 0.1875, ((0, 4), (2, 8)))
    w_out = noise(key_of[6], (SECTIONS, FF, D), FF ** -0.5, 0.03125, ((0, 4), (1, 8)))
    return dict(saved_inputs=saved_inputs, slot_index=slot_index, example_lengths=example_lengths, first_grads=first_grads, loss_grads=loss_grads, w_in=w_in, w_out=w_out)


GAMMA = 0.01

def membership(lengths, tokens):
    ends = jnp.cumsum(lengths)
    position = jnp.arange(tokens, dtype=jnp.int32)
    example_id = lax.optimization_barrier(jnp.sum((position[:, None] >= ends[None, :-1]).astype(jnp.int32), axis=1))
    labels = jnp.arange(lengths.shape[0], dtype=jnp.int32)
    return (example_id[:, None] == labels[None, :]).astype(jnp.float32)

def section_step(inputs, grads, first, second, lengths):
    z = jnp.dot(inputs, first, preferred_element_type=jnp.float32)
    relu = jnp.maximum(z, 0.0)
    hidden = (relu * relu).astype(jnp.bfloat16)
    back = jnp.dot(grads, second.T, preferred_element_type=jnp.float32)
    dz = (2.0 * relu * back).astype(jnp.bfloat16)
    dx = (grads.astype(jnp.float32) + jnp.dot(dz, first.T, preferred_element_type=jnp.float32)).astype(jnp.bfloat16)
    member = membership(lengths, inputs.shape[0])
    gram_x = jnp.dot(inputs, inputs.T, preferred_element_type=jnp.float32)
    gram_z = jnp.dot(dz, dz.T, preferred_element_type=jnp.float32)
    gram_h = jnp.dot(hidden, hidden.T, preferred_element_type=jnp.float32)
    gram_y = jnp.dot(grads, grads.T, preferred_element_type=jnp.float32)
    paired = gram_x * gram_z + gram_h * gram_y
    squares = lax.optimization_barrier(jnp.sum(member * jnp.dot(paired, member, precision=lax.Precision.HIGHEST), axis=0))
    factor = 1.0 / (jnp.sqrt(squares / (D * FF)) + GAMMA)
    token_factor = lax.optimization_barrier(jnp.sum(member * factor[None, :], axis=1))
    dzc = (dz.astype(jnp.float32) * token_factor[:, None]).astype(jnp.bfloat16)
    dyc = (grads.astype(jnp.float32) * token_factor[:, None]).astype(jnp.bfloat16)
    g_first = jnp.dot(inputs.T, dzc, preferred_element_type=jnp.float32)
    g_second = jnp.dot(hidden.T, dyc, preferred_element_type=jnp.float32)
    return (dx, g_first, g_second)

def reference(saved_inputs, slot_index, example_lengths, first_grads, loss_grads, w_in, w_out):
    section_count = w_in.shape[0]
    slot_count = slot_index.shape[1]
    acc_first = [jnp.zeros((D, FF), jnp.float32) for s in range(section_count)]
    acc_second = [jnp.zeros((FF, D), jnp.float32) for s in range(section_count)]
    previous = [None] * section_count
    results = [[None] * slot_count for s in range(section_count)]
    for slot in range(slot_count):
        current = [None] * section_count
        for section in range(section_count):
            if slot == 0:
                grads = first_grads[section]
            elif section == section_count - 1:
                grads = loss_grads[slot - 1]
            else:
                grads = previous[section + 1]
            inputs = lax.dynamic_index_in_dim(saved_inputs[section], slot_index[section, slot].astype(jnp.int32), 0, keepdims=False)
            dx, g_first, g_second = section_step(inputs, grads, w_in[section], w_out[section], example_lengths[section, slot])
            acc_first[section] = acc_first[section] + g_first
            acc_second[section] = acc_second[section] + g_second
            current[section] = dx
            results[section][slot] = dx
        previous = current
    grad_in = jnp.stack(acc_first).astype(jnp.bfloat16)
    grad_out = jnp.stack(acc_second).astype(jnp.bfloat16)
    input_grads = jnp.stack([jnp.stack(row) for row in results])
    return (grad_in, grad_out, input_grads)
```

```python
import jax
import jax.numpy as jnp
from jax import lax
from jax.sharding import PartitionSpec as P

GAMMA = 0.01
F32 = jnp.float32
BF16 = jnp.bfloat16


def shifted(value, axis, steps):
    count = lax.axis_size(axis)
    first, last = (max(0, -steps), min(count, count - steps))
    return lax.ppermute(value, axis, [(source, source + steps) for source in range(first, last)])


def membership(lengths, tokens):
    ends = jnp.cumsum(lengths)
    position = jnp.arange(tokens, dtype=jnp.int32)
    example_id = jnp.sum((position[:, None] >= ends[None, :-1]).astype(jnp.int32), axis=1)
    labels = jnp.arange(lengths.shape[0], dtype=jnp.int32)
    return (example_id[:, None] == labels[None, :]).astype(F32)


def spread(value, axis):
    copies = jnp.broadcast_to(value[None], (lax.axis_size(axis),) + value.shape)
    return lax.all_to_all(copies, axis, 0, 0)


def gram(value):
    return lax.dot_general(value, value, (((1,), (1,)), ((), ())), preferred_element_type=F32)


def per_device(saved_inputs, slot_index, example_lengths, first_grads, loss_grads, w_in, w_out):
    section_count = lax.axis_size("section")
    parts = lax.axis_size("tensor")
    is_last = lax.axis_index("section") == section_count - 1
    first = w_in[0]
    second = w_out[0]
    slot_count = loss_grads.shape[0] + 1
    rows, width = first_grads.shape[1:]
    hidden_all = first.shape[1] * parts
    picked = [
        lax.dynamic_index_in_dim(saved_inputs[0], slot_index[0, slot], 0, keepdims=False)
        for slot in range(slot_count)
    ]
    tokens = parts * rows
    opening = spread(jnp.concatenate([picked[0], first_grads[0]]), "tensor")
    later = spread(jnp.concatenate(picked[1:]), "tensor")
    every_input = [opening[:, :rows].reshape(tokens, width)]
    for slot in range(slot_count - 1):
        every_input.append(later[:, slot * rows : (slot + 1) * rows].reshape(tokens, width))
    incoming = first_grads[0]
    results, dzs, hiddens, grad_list, members, squares = [], [], [], [], [], []
    for slot in range(slot_count):
        inputs = every_input[slot]
        if slot == 0:
            grads = opening[:, rows:].reshape(tokens, width)
        else:
            grads = spread(incoming, "tensor").reshape(tokens, width)
        z = jnp.dot(inputs, first, preferred_element_type=F32)
        relu = jnp.maximum(z, 0.0)
        hidden = (relu * relu).astype(BF16)
        back = jnp.einsum("td,fd->tf", grads, second, preferred_element_type=F32)
        dz = (2.0 * relu * back).astype(BF16)
        own_terms = jnp.einsum("tf,df->td", dz, first, preferred_element_type=F32).astype(BF16)
        pieces = lax.all_to_all(own_terms.reshape(parts, rows, width), "tensor", 0, 0)
        shares = jnp.sum(pieces.astype(F32), axis=0)
        passing = (incoming.astype(F32) + shares).astype(BF16)
        results.append(passing)
        if slot + 1 < slot_count:
            arrived = shifted(passing, "section", -1)
            incoming = jnp.where(is_last, loss_grads[slot], arrived)
        member = membership(example_lengths[0, slot], inputs.shape[0])
        paired = gram(inputs) * gram(dz) + gram(hidden) * gram(grads)
        per_row = jnp.stack([jnp.sum(paired * member[:, e][None, :], axis=1) for e in range(member.shape[1])], axis=1)
        squares.append(jnp.sum(member * per_row, axis=0))
        dzs.append(dz)
        hiddens.append(hidden)
        grad_list.append(grads)
        members.append(member)
    local = jnp.stack(squares)
    total = jnp.sum(spread(local, "tensor"), axis=0)
    factor = 1.0 / (jnp.sqrt(total / (width * hidden_all)) + GAMMA)
    token_factor = jnp.concatenate([jnp.sum(m * factor[i][None, :], axis=1) for i, m in enumerate(members)])[:, None]
    xc = (jnp.concatenate(every_input).astype(F32) * token_factor).astype(BF16)
    dyc = (jnp.concatenate(grad_list).astype(F32) * token_factor).astype(BF16)
    grad_in = jnp.einsum("td,tf->df", xc, jnp.concatenate(dzs), preferred_element_type=F32).astype(BF16)[None]
    grad_out = jnp.einsum("tf,td->fd", jnp.concatenate(hiddens), dyc, preferred_element_type=F32).astype(BF16)[None]
    input_grads = jnp.stack(results)[None]
    return (grad_in, grad_out, input_grads)


def solution(mesh):
    return jax.shard_map(
        per_device,
        mesh=mesh,
        in_specs=(
            P("section", None, "tensor", None),
            P("section", None),
            P("section", None, None),
            P("section", "tensor", None),
            P(None, "tensor", None),
            P("section", None, "tensor"),
            P("section", "tensor", None),
        ),
        out_specs=(
            P("section", None, "tensor"),
            P("section", "tensor", None),
            P("section", None, "tensor", None),
        ),
        check_vma=False,
    )
```
